32 devices in a mesh: seq: 8 (over z, x), tp: 4 (over y, core).
Axes of the slice: x: 2, y: 2, z: 4, core: 2. Of those that a mesh axis runs over, the one named last changes fastest.
Arguments:
- queries: bfloat16 [1536, 4096], P('seq', 'tp'), may hold values from -80 to 80
- keys: bfloat16 [1536, 512], P('seq', 'tp'), may hold values from -4 to 4
- values: bfloat16 [1536, 512], P('seq', 'tp'), may hold values from -6 to 6
- segment_ids: int32 [1536], P('seq'), may hold values from 0 to 15, never falling along the last dimension, each value on 1 to 1152 neighbouring positions
- out_weight: bfloat16 [4096, 8192], P('tp', 'seq'), may hold values from -0.09375 to 0.09375
Outputs:
- projected: bfloat16 [1536, 8192], P('seq', 'tp')
The draws below stay inside these ranges and needn't reach their ends.
Inputs may be any that keep to these rules, and one draw needn't show every extreme that they name: `segment_ids`: segment numbers never fall along the sequence and every number from 0 to 15 occurs; no document has more than 1152 tokens and one has exactly that many.
All inputs are finite; a program needn't handle non-finite values.
Results may differ from the reference program's by a relative error of at most 0.012.
Values may be sent and summed in bfloat16 or wider, within the bound.
No kernel may reach another device: no remote copies, remote signals or barrier semaphores. Data moves between devices by JAX's collectives and lax.ppermute only.
A program may use at most 128 MiB of HBM per device.

```python
import math
import jax
import jax.numpy as jnp
import numpy as np
from jax import lax

HEADS = 32
KV_HEADS = 4
HEAD_DIM = 128
OUT_WIDTH = 8192
SEGMENTS = 16
TOKENS = 1536
N_TP = 4


def draw_key_field(key):
    base_draw = jax.random.normal(jax.random.fold_in(key, 11), (TOKENS, KV_HEADS * HEAD_DIM), jnp.float32)
    return jnp.clip(base_draw, -4.0, 4.0)


def draw_keys(key, part):
    return draw_key_field(key).astype(jnp.bfloat16)


def draw_queries(key, part):
    fresh_draw = 3.0 * jnp.clip(jax.random.normal(jax.random.fold_in(key, 12), (TOKENS, HEADS * HEAD_DIM), jnp.float32), -6.0, 6.0)
    return fresh_draw.astype(jnp.bfloat16)


def levels(stream_key, dims, pieces, low, top_value):
    level, own = 1.0, jax.random.fold_in(stream_key, 6)
    for dim, parts in pieces:
        heights = jnp.exp(jax.random.uniform(jax.random.fold_in(own, dim), (parts,), jnp.float32, low / len(pieces), top_value / len(pieces)))
        level = level * jnp.repeat(heights, dims[dim] // parts).reshape([-1 if axis == dim else 1 for axis in range(len(dims))])
    return level


def length_profile(amount, total, most, skew):
    loads = [(1 << 20) // math.isqrt(grade ** skew) + 1 for grade in range(2, amount + 1)]
    spare, given = total - most - (amount - 1), [1] * (amount - 1)
    while spare > 0:
        free = [i for i in range(amount - 1) if given[i] < most]
        whole, remaining = sum([loads[i] for i in free]), spare
        for i in free:
            extra = min(most - given[i], max(1, remaining * loads[i] // whole), spare)
            given[i] = given[i] + extra
            spare = spare - extra
    return np.array([most] + given)


def uneven(own_key, amount, total, reach, lean):
    if amount == 2:
        one = jax.random.randint(own_key, (), max(1, total - reach), min(reach, total - 1) + 1)
        return jnp.stack([one, total - one])
    sizes = jnp.asarray(length_profile(amount, total, reach, lean), jnp.int32)
    twos = (amount - 1) // 2
    donor, taker = sizes[1:1 + 2 * twos:2], sizes[2:2 + 2 * twos:2]
    slack = jnp.minimum(donor - 1, reach - taker)
    shifted = jax.random.randint(jax.random.fold_in(own_key, 1), (twos,), 0, 1 << 20) % (slack + 1)
    sizes = sizes.at[1:1 + 2 * twos:2].set(donor - shifted).at[2:2 + 2 * twos:2].set(taker + shifted)
    return sizes[jax.random.permutation(jax.random.fold_in(own_key, 2), amount)]


def centred(stream_key, extent, width, most, split=(), kind=jnp.bfloat16):
    result = jax.random.normal(stream_key, extent, jnp.float32) * width
    if len(split) > 0:
        result = levels(stream_key, extent, split, -0.22, 0.18) * result
    return jnp.clip(result, min=-most, max=most).astype(kind)


def setup_inputs(seed: int = 0) -> dict:
    splits = jax.random.split(jax.random.key(seed), 6)
    return {
        "queries": draw_queries(jax.random.fold_in(splits[5], 71), 0),
        "keys": draw_keys(jax.random.fold_in(splits[5], 71), 0),
        "values": centred(splits[2], (TOKENS, KV_HEADS * HEAD_DIM), 1.0, 6.0, ((0, 8), (1, 4))),
        "segment_ids": jnp.searchsorted(jnp.cumsum(uneven(splits[3], SEGMENTS, TOKENS, 3 * TOKENS // 4, 2)), jnp.arange(TOKENS), side="right").astype(jnp.int32),
        "out_weight": centred(splits[4], (HEADS * HEAD_DIM, OUT_WIDTH), (HEADS * HEAD_DIM) ** -0.5, 0.09375, ((0, 4), (1, 8))),
    }


rope_base = 500000.0
masked_score = -1e+30

def rotate_heads(inputs, positions, head_dim):
    row_count = inputs.shape[0]
    head_count = inputs.shape[1] // head_dim
    half_dim = head_dim // 2
    widened = inputs.astype(jnp.float32).reshape(row_count, head_count, head_dim)
    exponent = jnp.arange(half_dim, dtype=jnp.float32) * (2.0 / head_dim)
    inverse = jnp.power(jnp.float32(rope_base), -exponent)
    angles = positions.astype(jnp.float32)[:, None] * inverse[None, :]
    cosine_table = jnp.cos(angles)[:, None, :]
    sine_table = jnp.sin(angles)[:, None, :]
    first_half = widened[:, :, :half_dim]
    second_half = widened[:, :, half_dim:]
    turned = jnp.concatenate([first_half * cosine_table - second_half * sine_table, second_half * cosine_table + first_half * sine_table], axis=2)
    return turned.reshape(row_count, head_count * head_dim).astype(jnp.bfloat16)

def doc_counts_of(segment_ids, segments):
    labels = jnp.arange(segments, dtype=jnp.int32)
    return lax.optimization_barrier(jnp.sum((segment_ids[None, :] == labels[:, None]).astype(jnp.int32), axis=1))

def first_rows(segment, starts):
    labels = jnp.arange(starts.shape[0], dtype=jnp.int32)
    return lax.optimization_barrier(jnp.sum(jnp.where(segment[:, None] == labels[None, :], starts[None, :], 0), axis=1)).astype(jnp.int32)

def reference(queries, keys, values, segment_ids, out_weight):
    counts = doc_counts_of(segment_ids, SEGMENTS)
    doc_ends = jnp.cumsum(counts).astype(jnp.int32)
    starts = doc_ends - counts
    every_row = jnp.arange(TOKENS, dtype=jnp.int32)
    positions = every_row - first_rows(segment_ids, starts)
    query_rot = rotate_heads(queries, positions, HEAD_DIM)
    key_rot = rotate_heads(keys, positions, HEAD_DIM)
    group_size = HEADS // KV_HEADS
    score_scale = 1.0 / math.sqrt(HEAD_DIM)
    key_full = lax.optimization_barrier(key_rot).astype(jnp.float32).reshape(TOKENS, KV_HEADS, HEAD_DIM)
    value_full = values.astype(jnp.float32).reshape(TOKENS, KV_HEADS, HEAD_DIM)
    query_block = 128 if TOKENS % 128 == 0 else TOKENS

    def attend(block_number):
        first_row = block_number * query_block
        query_tile = lax.dynamic_slice_in_dim(query_rot, first_row, query_block, 0)
        query_tile = lax.optimization_barrier(query_tile).astype(jnp.float32).reshape(query_block, KV_HEADS, group_size, HEAD_DIM)
        query_rows = first_row + jnp.arange(query_block, dtype=jnp.int32)
        query_segs = lax.dynamic_slice_in_dim(segment_ids, first_row, query_block, 0)
        scores = jnp.einsum('tkgd,skd->kgts', query_tile, key_full, precision=lax.Precision.HIGHEST) * score_scale
        visible = (every_row[None, :] <= query_rows[:, None]) & (segment_ids[None, :] == query_segs[:, None])
        scores = jnp.where(visible[None, None], scores, masked_score)
        row_max = lax.optimization_barrier(jnp.max(scores, axis=-1, keepdims=True))
        weights_full = jnp.where(visible[None, None], jnp.exp(scores - row_max), 0.0)
        normalizer = lax.optimization_barrier(jnp.sum(weights_full, axis=-1))
        weights_low = lax.optimization_barrier(weights_full.astype(jnp.bfloat16)).astype(jnp.float32)
        numerator = jnp.einsum('kgts,skd->kgtd', weights_low, value_full, precision=lax.Precision.HIGHEST)
        output = numerator / normalizer[..., None]
        return jnp.transpose(output, (2, 0, 1, 3)).reshape(query_block, HEADS * HEAD_DIM).astype(jnp.bfloat16)
    attended = lax.map(attend, jnp.arange(TOKENS // query_block, dtype=jnp.int32)).reshape(TOKENS, HEADS * HEAD_DIM)
    head_width = HEADS * HEAD_DIM // N_TP
    summed = jnp.zeros((TOKENS, OUT_WIDTH), jnp.float32)
    for shard in range(N_TP):
        term = jnp.dot(attended[:, shard * head_width:(shard + 1) * head_width], out_weight[shard * head_width:(shard + 1) * head_width], preferred_element_type=jnp.float32).astype(jnp.bfloat16)
        summed = summed + lax.optimization_barrier(term).astype(jnp.float32)
    return summed.astype(jnp.bfloat16)
```

```python
import functools
import math

import jax
import jax.numpy as jnp
from jax import lax
from jax.experimental import pallas as pl
from jax.experimental.pallas import tpu as pltpu
from jax.sharding import Mesh, PartitionSpec as P

HEADS = 32
KV_HEADS = 4
HEAD_DIM = 128
SEGMENTS = 16

rope_base = 500000.0
masked_score = -1e30
INFO_ROWS = 16
BASE = 128


def doc_counts_of(segment_ids, segments):
    labels = jnp.arange(segments, dtype=jnp.int32)
    return jnp.sum((segment_ids[None, :] == labels[:, None]).astype(jnp.int32), axis=1)


def largest_divisor(total, candidates):
    for candidate in candidates:
        if total % candidate == 0:
            return candidate
    return total


def rotary_tables(positions):
    half = HEAD_DIM // 2
    exponent = jnp.arange(half, dtype=jnp.float32) * (2.0 / HEAD_DIM)
    inverse = jnp.power(jnp.float32(rope_base), -exponent)
    angles = positions.astype(jnp.float32)[:, None] * inverse[None, :]
    cosine = jnp.cos(angles)
    sine = jnp.sin(angles)
    return (
        jnp.concatenate([cosine, cosine], axis=1),
        jnp.concatenate([-sine, sine], axis=1),
    )


def attend_kernel(
    scalars,
    queries,
    cosine,
    sine,
    keys,
    values,
    out,
    stacked,
    top,
    total,
    numerator,
    *,
    tile_q,
    tile_k,
    heads,
    segments,
):
    tile = pl.program_id(0)
    first = scalars[0] + tile * tile_q
    low = jnp.int32(0)
    for g in range(segments):
        end = scalars[1 + g]
        low = jnp.maximum(low, jnp.where(end <= first, end, 0))
    rows = first + lax.broadcasted_iota(jnp.int32, (tile_q, tile_k), 0)
    starts = jnp.zeros((tile_q, tile_k), jnp.int32)
    for g in range(segments):
        end = scalars[1 + g]
        starts = jnp.maximum(starts, jnp.where(end <= rows, end, 0))
    cos_tile = cosine[...]
    sin_tile = sine[...]
    for h in range(heads):
        x = queries[:, h * HEAD_DIM : (h + 1) * HEAD_DIM].astype(jnp.float32)
        turned = x * cos_tile + pltpu.roll(x, HEAD_DIM // 2, 1) * sin_tile
        stacked[h * tile_q : (h + 1) * tile_q, :] = turned.astype(jnp.bfloat16)
    top[...] = jnp.full(top.shape, masked_score, jnp.float32)
    total[...] = jnp.zeros(total.shape, jnp.float32)
    numerator[...] = jnp.zeros(numerator.shape, jnp.float32)
    scale = math.log2(math.e) / math.sqrt(HEAD_DIM)
    last_tile = (first + tile_q - 1) // tile_k
    first_tile = low // tile_k
    lanes = lax.broadcasted_iota(jnp.int32, (tile_q, tile_k), 1)

    def step(index, carry):
        offset = pl.multiple_of((last_tile - index) * tile_k, tile_k)
        key_tile = keys[pl.ds(offset, tile_k), :]
        value_tile = values[pl.ds(offset, tile_k), :]
        scores = lax.dot_general(
            stacked[...], key_tile, (((1,), (1,)), ((), ())), preferred_element_type=jnp.float32
        )
        columns = offset + lanes
        visible = (columns <= rows) & (columns >= starts)
        scores = jnp.where(visible[None], scores.reshape(heads, tile_q, tile_k), masked_score)
        scores = scores.reshape(heads * tile_q, tile_k)
        old = top[...]
        new = jnp.maximum(old, jnp.max(scores, axis=1, keepdims=True))
        rescale = jnp.exp2((old - new) * scale)
        weights = jnp.exp2((scores - new) * scale)
        total[...] = total[...] * rescale + jnp.sum(weights, axis=1, keepdims=True)
        numerator[...] = numerator[...] * rescale + jnp.dot(
            weights.astype(jnp.bfloat16), value_tile, preferred_element_type=jnp.float32
        )
        top[...] = new
        return carry

    lax.fori_loop(0, last_tile - first_tile + 1, step, 0)
    result = numerator[...] / total[...]
    for h in range(heads):
        out[:, h * HEAD_DIM : (h + 1) * HEAD_DIM] = result[h * tile_q : (h + 1) * tile_q, :].astype(
            jnp.bfloat16
        )


def attend(scalars, queries, cosine, sine, keys, values):
    row_count, width = queries.shape
    heads = width // HEAD_DIM
    key_count = keys.shape[0]
    tile_q = largest_divisor(row_count, (64, 32, 16))
    tile_k = largest_divisor(key_count, (256, 128))
    segments = scalars.shape[0] - 1
    kernel = functools.partial(
        attend_kernel, tile_q=tile_q, tile_k=tile_k, heads=heads, segments=segments
    )
    whole = pl.BlockSpec((key_count, HEAD_DIM), lambda i, s: (0, 0))
    pairs = row_count * key_count * heads // 3
    return pl.pallas_call(
        kernel,
        out_shape=jax.ShapeDtypeStruct((row_count, width), jnp.bfloat16),
        grid_spec=pltpu.PrefetchScalarGridSpec(
            num_scalar_prefetch=1,
            grid=(row_count // tile_q,),
            in_specs=[
                pl.BlockSpec((tile_q, width), lambda i, s: (i, 0)),
                pl.BlockSpec((tile_q, HEAD_DIM), lambda i, s: (i, 0)),
                pl.BlockSpec((tile_q, HEAD_DIM), lambda i, s: (i, 0)),
                whole,
                whole,
            ],
            out_specs=pl.BlockSpec((tile_q, width), lambda i, s: (i, 0)),
            scratch_shapes=[
                pltpu.VMEM((heads * tile_q, HEAD_DIM), jnp.bfloat16),
                pltpu.VMEM((heads * tile_q, 1), jnp.float32),
                pltpu.VMEM((heads * tile_q, 1), jnp.float32),
                pltpu.VMEM((heads * tile_q, HEAD_DIM), jnp.float32),
            ],
        ),
        cost_estimate=pl.CostEstimate(
            flops=4 * pairs * HEAD_DIM,
            bytes_accessed=4 * row_count * width + 4 * key_count * HEAD_DIM,
            transcendentals=pairs,
        ),
        name="attend",
    )(scalars, queries, cosine, sine, keys, values)


def local(queries, keys, values, segment_ids, out_weight, *, outer, inner, groups):
    row_count = queries.shape[0]
    width = queries.shape[1]
    z = lax.axis_index("outer")
    x = lax.axis_index("inner")
    k = lax.axis_index("tp")

    counts = doc_counts_of(segment_ids, SEGMENTS)
    info = jnp.concatenate([counts // BASE, counts % BASE]).astype(jnp.bfloat16)
    info = jnp.pad(info[None, :], ((0, INFO_ROWS - 1), (0, HEAD_DIM - 2 * SEGMENTS)))
    own = jnp.concatenate([keys, values, info], axis=0)
    block_rows = own.shape[0]

    def shift(array, axis, size, distance):
        pairs = [(i, (i - distance) % size) for i in range(size)]
        return lax.ppermute(array, axis, pairs)

    near = jnp.zeros((inner, block_rows, HEAD_DIM), jnp.bfloat16)
    near = lax.dynamic_update_slice(near, own[None], (x, 0, 0))
    for d in range(1, inner):
        got = shift(own, "inner", inner, d)
        near = lax.dynamic_update_slice(near, got[None], ((x + d) % inner, 0, 0))
    weights = [out_weight]
    for d in range(1, inner):
        weights.append(shift(out_weight, "inner", inner, d))

    every = jnp.zeros((outer, inner, block_rows, HEAD_DIM), jnp.bfloat16)
    every = lax.dynamic_update_slice(every, near[None], (z, 0, 0, 0))
    for d in range(1, outer):
        got = shift(near, "outer", outer, d)
        every = lax.dynamic_update_slice(every, got[None], ((z + d) % outer, 0, 0, 0))
    every = every.reshape(outer * inner, block_rows, HEAD_DIM)
    query_blocks = [queries] + [shift(queries, "outer", outer, d) for d in range(1, outer)]

    info = every[:, 2 * row_count, :].astype(jnp.float32)
    block_counts = info[:, :SEGMENTS] * BASE + info[:, SEGMENTS : 2 * SEGMENTS]
    totals = jnp.sum(block_counts, axis=0).astype(jnp.int32)
    labels = jnp.arange(SEGMENTS, dtype=jnp.int32)
    doc_ends = jnp.sum(jnp.where(labels[None, :] <= labels[:, None], totals[None, :], 0), axis=1)
    token_count = outer * inner * row_count
    tokens = jnp.arange(token_count, dtype=jnp.int32)
    doc_starts = jnp.max(
        jnp.where(doc_ends[None, :] <= tokens[:, None], doc_ends[None, :], 0), axis=1
    )
    cosine, sine = rotary_tables(tokens - doc_starts)
    raw_keys = every[:, :row_count, :].reshape(token_count, HEAD_DIM).astype(jnp.float32)
    swapped = jnp.concatenate([raw_keys[:, HEAD_DIM // 2 :], raw_keys[:, : HEAD_DIM // 2]], axis=1)
    key_rot = (raw_keys * cosine + swapped * sine).astype(jnp.bfloat16)
    value_all = every[:, row_count : 2 * row_count, :].reshape(token_count, HEAD_DIM)

    attended = []
    for d in range(outer):
        first = (((z + d) % outer) * inner + x) * row_count
        scalars = jnp.concatenate([first[None].astype(jnp.int32), doc_ends])
        cos_rows = lax.dynamic_slice_in_dim(cosine, first, row_count, 0)
        sin_rows = lax.dynamic_slice_in_dim(sine, first, row_count, 0)
        attended.append(attend(scalars, query_blocks[d], cos_rows, sin_rows, key_rot, value_all))
    attended = jnp.stack(attended)

    def project(weight):
        blocks = attended
        bit = 1
        size = groups
        partial = None
        while bit < groups:
            mine = (k // bit) % 2
            if partial is None:
                paired = blocks.reshape(size // 2, 2, row_count, width)
                give = lax.dynamic_index_in_dim(paired, 1 - mine, 1, keepdims=False)
                keep = lax.dynamic_index_in_dim(paired, mine, 1, keepdims=False)

                def times(rows):
                    flat = rows.reshape(-1, width)
                    return jnp.dot(flat, weight, preferred_element_type=jnp.float32)

                given = times(give).astype(jnp.bfloat16)
                kept = times(keep)
            else:
                paired = partial.reshape(size // 2, 2, row_count, -1)
                give = lax.dynamic_index_in_dim(paired, 1 - mine, 1, keepdims=False)
                kept = lax.dynamic_index_in_dim(paired, mine, 1, keepdims=False)
                given = give.astype(jnp.bfloat16).reshape(size // 2 * row_count, -1)
                kept = kept.reshape(size // 2 * row_count, -1)
            got = lax.ppermute(given, "tp", [(i, i ^ bit) for i in range(groups)])
            partial = kept.astype(jnp.bfloat16).astype(jnp.float32) + got.astype(jnp.float32)
            size = size // 2
            bit = bit * 2
        moves = []
        for a in range(outer):
            for b in range(groups):
                moves.append((a * groups + b, ((a + b) % outer) * groups + a))
        return lax.ppermute(partial.astype(jnp.bfloat16), ("outer", "tp"), moves)

    pieces = [project(weights[0])]
    if inner > 1:
        pieces.append(project(jnp.concatenate(weights[1:], axis=1)))
    relative = jnp.concatenate(pieces, axis=1)
    if inner == 1:
        return relative
    columns = out_weight.shape[1]
    if inner == 2:
        turned = jnp.concatenate([relative[:, columns:], relative[:, :columns]], axis=1)
        return jnp.where(x == 0, relative, turned)
    doubled = jnp.concatenate([relative, relative], axis=1)
    offset = ((inner - x) % inner) * columns
    return lax.dynamic_slice_in_dim(doubled, offset, inner * columns, 1)


def solution(mesh):
    seq, groups = mesh.shape["seq"], mesh.shape["tp"]
    outer, inner = groups, seq // groups
    split = Mesh(mesh.devices.reshape(outer, inner, groups), ("outer", "inner", "tp"))
    whole = ("outer", "inner")
    return jax.shard_map(
        functools.partial(local, outer=outer, inner=inner, groups=groups),
        mesh=split,
        in_specs=(P(whole, "tp"), P(whole, "tp"), P(whole, "tp"), P(whole), P("tp", whole)),
        out_specs=P(whole, "tp"),
        check_vma=False,
    )
```
